32 devices in a mesh: gx: 8 (over z, y), gy: 4 (over x, core).
Axes of the slice: x: 2, y: 2, z: 4, core: 2. Of those that a mesh axis runs over, the one named last changes fastest.
Arguments:
- right_side: float32 [128, 256, 512], P('gx', 'gy'), may hold values from -8 to 8
- guess: float32 [128, 256, 512], P('gx', 'gy'), may hold values from -4 to 4
- diagonal: float32 [128, 256, 512], P('gx', 'gy'), may hold values from 0.02 to 0.5
Outputs:
- solution_field: float32 [128, 256, 512], P('gx', 'gy')
- residual: float32 [128, 256, 512], P('gx', 'gy')
The draws below stay inside these ranges and needn't reach their ends.
All inputs are finite; a program needn't handle non-finite values.
Results may differ from the reference program's by a relative error of at most 0.00065.
Values sent between devices are 32-bit elements; how exact they have to be, the bound alone decides.
A program may use at most 128 MiB of HBM per device.

```python
import math
import jax
import jax.numpy as jnp
from jax import lax

NZ = 512
STEPS = 4
NX = 128
NY = 256


def level_of(rng, extent, cuts, smallest, largest):
    def one(position, parts):
        draws = jax.random.uniform(jax.random.fold_in(jax.random.fold_in(rng, 6), position), (parts,), jnp.float32, smallest / len(cuts), largest / len(cuts))
        return jnp.repeat(jnp.exp(draws), extent[position] // parts).reshape((-1,) + (1,) * (len(extent) - position - 1))

    gain = one(*cuts[0])
    for cut in cuts[1:]:
        gain = gain * one(*cut)
    return gain


def normal_values(own_key, dims, deviation, reach, cuts=(), held_as=jnp.bfloat16):
    drawn = jax.random.normal(own_key, dims, jnp.float32) * deviation
    if len(cuts) > 0:
        drawn = level_of(own_key, dims, cuts, -0.22, 0.18) * drawn
    return jnp.clip(drawn, min=-reach, max=reach).astype(held_as)


def setup_inputs(seed: int = 0) -> dict:
    splits = jax.random.split(jax.random.key(seed), 4)
    return {
        "right_side": normal_values(splits[0], (NX, NY, NZ), 1.0, 8.0, ((0, 8), (1, 4)), jnp.float32),
        "guess": normal_values(splits[1], (NX, NY, NZ), 0.5, 4.0, ((0, 8), (1, 4)), jnp.float32),
        "diagonal": jnp.clip(jnp.exp(math.log(0.5) - 3.218876 * jax.random.uniform(splits[2], (NX, NY, NZ), jnp.float32) ** level_of(splits[2], (NX, NY, NZ), ((0, 8), (1, 4)), -0.2, 0.2)), 0.02, 0.5),
    }


center_shift = 6.25
half_range = 6.25


def operate(field, diagonal):
    padded = jnp.pad(field, 1)
    beside = padded[2:, 1:-1, 1:-1] + padded[:-2, 1:-1, 1:-1]
    beside = beside + padded[1:-1, 2:, 1:-1] + padded[1:-1, :-2, 1:-1]
    beside = beside + padded[1:-1, 1:-1, 2:] + padded[1:-1, 1:-1, :-2]
    return (6.0 + diagonal) * field - beside


def change_matrix(depth):
    rows = []
    for i in range(depth + 1):
        line = []
        for k in range(depth + 1):
            value = 0.0
            if k == 0:
                value = center_shift if i == 0 else (half_range if i == 1 else 0.0)
            elif k < depth:
                if i == k:
                    value = center_shift
                elif i == k - 1 or i == k + 1:
                    value = half_range / 2.0
            line.append(value)
        rows.append(line)
    return jnp.array(rows, dtype=jnp.float32)


def quad(left, matrix, right):
    return jnp.sum(left * jnp.dot(matrix, right, precision=lax.Precision.HIGHEST))


def coefficient_steps(gram, depth):
    change = change_matrix(depth)
    unit = jnp.zeros((depth + 1,), jnp.float32).at[0].set(1.0)
    xc = jnp.zeros((depth + 1,), jnp.float32)
    rc = unit
    pc = unit
    for step in range(depth):
        rr = quad(rc, gram, rc)
        moved = jnp.dot(change, pc, precision=lax.Precision.HIGHEST)
        alpha = rr / quad(pc, gram, moved)
        xc = xc + alpha * pc
        rc = rc - alpha * moved
        beta = quad(rc, gram, rc) / rr
        pc = rc + beta * pc
    return xc, rc


def reference(right_side, guess, diagonal):
    first = right_side - operate(guess, diagonal)
    basis = [first]
    for k in range(STEPS):
        applied = operate(basis[k], diagonal)
        if k == 0:
            nextone = (applied - center_shift * basis[k]) / half_range
        else:
            nextone = 2.0 * (applied - center_shift * basis[k]) / half_range - basis[k - 1]
        basis.append(nextone)
    stacked = jnp.stack(basis).reshape(STEPS + 1, -1)
    gram = jnp.dot(stacked, stacked.T, precision=lax.Precision.HIGHEST)
    xc, rc = coefficient_steps(gram, STEPS)
    solution_field = guess
    residual = jnp.zeros_like(guess)
    for k in range(STEPS + 1):
        solution_field = solution_field + xc[k] * basis[k]
        residual = residual + rc[k] * basis[k]
    return solution_field, residual
```

```python
import functools
import jax
import jax.numpy as jnp
from jax import lax
from jax.experimental import pallas as pl
from jax.experimental.pallas import tpu as pltpu
from jax.sharding import PartitionSpec as P

STEPS = 4
center_shift = 6.25
half_range = 6.25
PAD = 8
MESH = pl.DeviceIdType.MESH


def change_matrix(depth):
    rows = []
    for i in range(depth + 1):
        line = []
        for k in range(depth + 1):
            value = 0.0
            if k == 0:
                value = center_shift if i == 0 else half_range if i == 1 else 0.0
            elif k < depth:
                if i == k:
                    value = center_shift
                elif i == k - 1 or i == k + 1:
                    value = half_range / 2.0
            line.append(value)
        rows.append(line)
    return rows


def total(terms):
    terms = list(terms)
    while len(terms) > 1:
        pairs = [a + b for a, b in zip(terms[::2], terms[1::2])]
        terms = pairs + ([terms[-1]] if len(terms) % 2 else [])
    return terms[0]


def quad(left, gram, right):
    return total(l * total(g * r for g, r in zip(line, right)) for l, line in zip(left, gram))


def coefficient_steps(gram, depth, zero, one):
    change = change_matrix(depth)
    unit = [one] + [zero] * depth
    xc, rc, pc = [zero] * (depth + 1), unit, unit
    rr = quad(rc, gram, rc)
    for step in range(depth):
        moved = []
        for line in change:
            terms = [c * p for c, p in zip(line, pc) if c != 0.0]
            moved.append(total(terms))
        alpha = rr / quad(pc, gram, moved)
        xc = [x + alpha * p for x, p in zip(xc, pc)]
        rc = [r - alpha * m for r, m in zip(rc, moved)]
        new = quad(rc, gram, rc)
        beta = new / rr
        pc = [r + beta * p for r, p in zip(rc, pc)]
        rr = new
    return xc, rc


def fold(p):
    rows, cols = p.shape
    return total(
        p[i : i + 8, j : j + 128] for i in range(0, rows, 8) for j in range(0, cols, 128)
    )


def kernel(px, py, rows, r_hbm, g_hbm, d_hbm, sol_hbm, res_hbm,
           F, R, D, Ys, Yr, A, M1, M2, acc,
           load_sem, xs_sem, xr_sem, ys_sem, yr_sem, as_sem, a1_sem, a2_sem, out_sem):
    LX, LY, LZ = R.shape
    NC = LY // rows
    gx, gy = lax.axis_index("gx"), lax.axis_index("gy")
    low_x, high_x, low_y, high_y = gx > 0, gx < px - 1, gy > 0, gy < py - 1
    inner = pl.ds(PAD, LY)

    loads = [
        pltpu.make_async_copy(g_hbm, F.at[0, pl.ds(1, LX), inner, :], load_sem.at[0]),
        pltpu.make_async_copy(d_hbm, D, load_sem.at[1]),
        pltpu.make_async_copy(r_hbm, R, load_sem.at[2]),
    ]
    for copy in loads:
        copy.start()

    barrier = pltpu.get_barrier_semaphore()
    for o in range(1, px):
        pl.semaphore_signal(barrier, inc=1, device_id={"gx": lax.rem(gx + o, px)}, device_id_type=MESH)
    for o in range(1, py):
        pl.semaphore_signal(barrier, inc=1, device_id={"gy": lax.rem(gy + o, py)}, device_id_type=MESH)

    def zero_planes(x):
        def one(j, carry):
            at = pl.multiple_of(PAD + j * 8, 8)
            for k in range(STEPS + 1):
                F[k, x, pl.ds(at, 8), :] = jnp.zeros((8, LZ), jnp.float32)
            return carry
        lax.fori_loop(0, LY // 8, one, 0)

    pl.when(jnp.logical_not(low_x))(lambda: zero_planes(0))
    pl.when(jnp.logical_not(high_x))(lambda: zero_planes(LX + 1))

    def zero_rows(side):
        for k in range(STEPS + 1):
            Yr[k, side] = jnp.zeros((LX, LZ), jnp.float32)

    pl.when(jnp.logical_not(low_y))(lambda: zero_rows(0))
    pl.when(jnp.logical_not(high_y))(lambda: zero_rows(1))

    pl.semaphore_wait(barrier, px + py - 2)

    def x_copy(k, side, j):
        at = pl.ds(PAD + j * rows, rows)
        if k == 0:
            src = g_hbm.at[0 if side == 0 else LX - 1, pl.ds(j * rows, rows), :]
        else:
            src = F.at[k, 1 if side == 0 else LX, at, :]
        return pltpu.make_async_remote_copy(
            src_ref=src,
            dst_ref=F.at[k, LX + 1 if side == 0 else 0, at, :],
            send_sem=xs_sem.at[k, side, j],
            recv_sem=xr_sem.at[k, side, j],
            device_id={"gx": gx - 1 if side == 0 else gx + 1},
            device_id_type=MESH,
        )

    def y_copy(k, side):
        return pltpu.make_async_remote_copy(
            src_ref=Ys.at[k, side],
            dst_ref=Yr.at[k, 1 - side],
            send_sem=ys_sem.at[k, side],
            recv_sem=yr_sem.at[k, side],
            device_id={"gy": gy - 1 if side == 0 else gy + 1},
            device_id_type=MESH,
        )

    x_has, y_has = (low_x, high_x), (low_y, high_y)

    def send_x(k, j):
        for side in (0, 1):
            pl.when(x_has[side])(lambda: x_copy(k, side, j).start())

    def wait_x(k, j):
        for side in (0, 1):
            pl.when(x_has[1 - side])(lambda: x_copy(k, side, j).wait_recv())

    def send_y(k):
        for x in range(LX):
            Ys[k, 0, x : x + 1, :] = F[k, x + 1, PAD : PAD + 1, :]
            Ys[k, 1, x : x + 1, :] = F[k, x + 1, PAD + LY - 1 : PAD + LY, :]
        for side in (0, 1):
            pl.when(y_has[side])(lambda: y_copy(k, side).start())

    def wait_y(k):
        for side in (0, 1):
            pl.when(y_has[1 - side])(lambda: y_copy(k, side).wait_recv())
        for x in range(LX):
            F[k, x + 1, PAD - 1 : PAD, :] = Yr[k, 0, x : x + 1, :]
            F[k, x + 1, PAD + LY : PAD + LY + 1, :] = Yr[k, 1, x : x + 1, :]

    order = [0] + ([NC - 1] if NC > 1 else []) + list(range(1, NC - 1))
    for j in order:
        send_x(0, j)

    acc[...] = jnp.zeros(acc.shape, jnp.float32)
    zero_tile = jnp.zeros((8, 128), jnp.float32)

    def block(k, x, y, n):
        here = F[k - 1, x, PAD + y : PAD + y + n, :]
        lane = lax.broadcasted_iota(jnp.int32, (n, LZ), 1)
        at = pl.ds(PAD + y, n)
        beside = F[k - 1, x + 1, at, :] + F[k - 1, x - 1, at, :]
        beside = beside + (F[k - 1, x, pl.ds(PAD + y + 1, n), :] + F[k - 1, x, pl.ds(PAD + y - 1, n), :])
        beside = beside + jnp.where(lane == LZ - 1, 0.0, pltpu.roll(here, LZ - 1, 1))
        beside = beside + jnp.where(lane == 0, 0.0, pltpu.roll(here, 1, 1))
        diag = D[x - 1, pl.ds(y, n), :]
        if k == 1:
            new = R[x - 1, pl.ds(y, n), :] - ((6.0 + diag) * here - beside)
        elif k == 2:
            new = ((diag + (6.0 - center_shift)) * here - beside) * (1.0 / half_range)
        else:
            new = ((diag + (6.0 - center_shift)) * here - beside) * (2.0 / half_range) - F[k - 2, x, at, :]
        F[k, x, at, :] = new
        return fold(new * new), (fold(new * here) if k > 1 else zero_tile)

    def add(a, b):
        return a[0] + b[0], a[1] + b[1]

    loads[0].wait()
    send_y(0)
    loads[1].wait()
    loads[2].wait()

    for k in range(1, STEPS + 2):
        sums = (zero_tile, zero_tile)
        wait_y(k - 1)
        for i, j in enumerate(order):
            wait_x(k - 1, j)
            for x in (1, LX):
                sums = add(sums, block(k, x, j * rows, rows))
            if k <= STEPS:
                send_x(k, j)
            if i == 1 and k <= STEPS:
                send_y(k)
            if i == 0:
                spans = [(0, 8), (LY - 8, 8)]
            elif i < NC - 1:
                spans = [(8 + (i - 1) * rows, rows)]
            else:
                spans = [(8 + (i - 1) * rows, LY - 16 - (i - 1) * rows)]

            def plane(x, s):
                for y, n in spans:
                    s = add(s, block(k, x, y, n))
                return s

            sums = lax.fori_loop(2, LX, plane, sums, unroll=2)
        acc[2 * (k - 1)] = sums[0]
        if k > 1:
            acc[2 * (k - 1) - 1] = sums[1]

    lane = lax.broadcasted_iota(jnp.int32, (1, 128), 1)
    row = jnp.zeros((1, 128), jnp.float32)
    count = 2 * STEPS + 1
    for m in range(count):
        s = jnp.sum(jnp.sum(acc[m], axis=0, keepdims=True), axis=1, keepdims=True)
        row = row + jnp.where(lane == m, s, 0.0)

    def exchange(stage, axis, me, peers, slots, sems, row):
        A[stage] = row
        copies = [
            pltpu.make_async_remote_copy(
                src_ref=A.at[stage], dst_ref=slots.at[o - 1],
                send_sem=as_sem.at[stage, o - 1], recv_sem=sems.at[o - 1],
                device_id={axis: lax.rem(me + o, peers)}, device_id_type=MESH,
            )
            for o in range(1, peers)
        ]
        for copy in copies:
            copy.start()
        for copy in copies:
            copy.wait_recv()
        row = total([row] + [slots[o] for o in range(peers - 1)])
        return row, copies

    row, first = exchange(0, "gy", gy, py, M1, a1_sem, row)
    row, second = exchange(1, "gx", gx, px, M2, a2_sem, row)

    got = [
        jnp.broadcast_to(jnp.sum(jnp.where(lane == m, row, 0.0), axis=1, keepdims=True), (8, 128))
        for m in range(count)
    ]
    moments = []
    for m in range(count):
        moments.append(got[m] if m < 2 else 2.0 * got[m] - got[m % 2])
    gram = [
        [0.5 * (moments[i + j] + moments[abs(i - j)]) for j in range(STEPS + 1)]
        for i in range(STEPS + 1)
    ]
    xc, rc = coefficient_steps(gram, STEPS, jnp.zeros((8, 128), jnp.float32), jnp.ones((8, 128), jnp.float32))
    wide = [[jnp.concatenate([c] * (LZ // 128), axis=1) for c in cs] for cs in (xc, rc)]

    slabs = 4 if LX % 4 == 0 else 1
    per = LX // slabs
    outs = []
    for s in range(slabs):
        def plane(x, carry):
            def strip(i, carry):
                y = pl.multiple_of(i * 8, 8)
                at = pl.ds(pl.multiple_of(PAD + y, 8), 8)
                sol = F[0, x + 1, at, :]
                res = jnp.zeros((8, LZ), jnp.float32)
                for k in range(STEPS + 1):
                    b = F[k + 1, x + 1, at, :]
                    sol = sol + wide[0][k] * b
                    res = res + wide[1][k] * b
                R[x, pl.ds(y, 8), :] = sol
                D[x, pl.ds(y, 8), :] = res
                return carry
            return lax.fori_loop(0, LY // 8, strip, carry, unroll=4)

        lax.fori_loop(s * per, (s + 1) * per, plane, 0)
        at = pl.ds(s * per, per)
        for i, (src, dst) in enumerate(((R, sol_hbm), (D, res_hbm))):
            copy = pltpu.make_async_copy(src.at[at], dst.at[at], out_sem.at[i, s])
            copy.start()
            outs.append(copy)

    for k in range(STEPS + 1):
        for side in (0, 1):
            def done():
                for j in range(NC):
                    x_copy(k, side, j).wait_send()
            pl.when(x_has[side])(done)
            pl.when(y_has[side])(lambda: y_copy(k, side).wait_send())
    for copy in first + second:
        copy.wait_send()
    for copy in outs:
        copy.wait()


def solution(mesh):
    px, py = mesh.shape["gx"], mesh.shape["gy"]

    def shards(right_side, guess, diagonal):
        LX, LY, LZ = guess.shape
        rows = 16
        NC = LY // rows
        n = STEPS + 1
        dma = pltpu.SemaphoreType.DMA
        like = jax.ShapeDtypeStruct(guess.shape, jnp.float32)
        return pl.pallas_call(
            functools.partial(kernel, px, py, rows),
            out_shape=(like, like),
            in_specs=[pl.BlockSpec(memory_space=pl.ANY)] * 3,
            out_specs=(pl.BlockSpec(memory_space=pl.ANY),) * 2,
            scratch_shapes=[
                pltpu.VMEM((n + 1, LX + 2, LY + 2 * PAD, LZ), jnp.float32),
                pltpu.VMEM((LX, LY, LZ), jnp.float32),
                pltpu.VMEM((LX, LY, LZ), jnp.float32),
                pltpu.VMEM((n, 2, LX, LZ), jnp.float32),
                pltpu.VMEM((n, 2, LX, LZ), jnp.float32),
                pltpu.VMEM((2, 1, 128), jnp.float32),
                pltpu.VMEM((py - 1, 1, 128), jnp.float32),
                pltpu.VMEM((px - 1, 1, 128), jnp.float32),
                pltpu.VMEM((2 * STEPS + 1, 8, 128), jnp.float32),
                dma((3,)), dma((n, 2, NC)), dma((n, 2, NC)), dma((n, 2)), dma((n, 2)),
                dma((2, max(px, py) - 1)), dma((py - 1,)), dma((px - 1,)), dma((2, 4)),
            ],
            compiler_params=pltpu.CompilerParams(
                collective_id=0, has_side_effects=True, vmem_limit_bytes=48 * 1024 * 1024
            ),
        )(right_side, guess, diagonal)

    spec = P("gx", "gy", None)
    return jax.shard_map(
        shards, mesh=mesh, in_specs=(spec,) * 3, out_specs=(spec,) * 2, check_vma=False
    )
```
